32 devices in a mesh: lat: 8 (over z, y), lon: 4 (over x, core).
Axes of the slice: x: 2, y: 2, z: 4, core: 2. Of those that a mesh axis runs over, the one named last changes fastest.
Arguments:
- raw_fields: bfloat16 [32, 160, 1440], P(('lat', 'lon')), may hold values from -6 to 6
- embed_weight: bfloat16 [32, 4, 4, 1024], replicated, may hold values from -0.25 to 0.25
- embed_bias: float32 [1024], replicated, may hold values from -3 to 3
- conv_weight: bfloat16 [3, 3, 1024, 1024], replicated, may hold values from -0.0625 to 0.0625
- conv_bias: float32 [1024], replicated, may hold values from -3 to 3
Outputs:
- features: bfloat16 [40, 360, 1024], P('lat', 'lon')
The draws below stay inside these ranges and needn't reach their ends.
All inputs are finite; a program needn't handle non-finite values.
Results may differ from the reference program's by a relative error of at most 0.0049.
Values may be sent and summed in bfloat16 or wider, within the bound.
A program may use at most 192 MiB of HBM per device.

```python
import jax
import jax.numpy as jnp

PATCH = 4
WIDTH = 1024
VARS = 32
HEIGHT = 160
BREADTH = 1440


def shard_levels(key, extent, split, least, top_value):
    level = 1.0
    for dim, shards_of in split:
        heights = jax.random.uniform(jax.random.fold_in(jax.random.fold_in(key, 6), dim), (shards_of,), jnp.float32, least / len(split), top_value / len(split))
        level = level * jnp.repeat(jnp.exp(heights), extent[dim] // shards_of).reshape((-1,) + (1,) * (len(extent) - 1 - dim))
    return level


def gaussian(own_key, dims, scale, most, pieces=(), kind=jnp.bfloat16):
    gain = shard_levels(own_key, dims, pieces, -0.22, 0.18) if pieces else 1.0
    values = jax.random.normal(own_key, dims, jnp.float32) * scale * gain
    return jnp.minimum(jnp.maximum(values, -most), most).astype(kind)


def setup_inputs(seed: int = 0) -> dict:
    arg_keys = jax.random.split(jax.random.key(seed), 6)
    return {
        "raw_fields": gaussian(arg_keys[0], (VARS, HEIGHT, BREADTH), 1.0, 6.0, ((0, 32),)),
        "embed_weight": gaussian(arg_keys[1], (VARS, PATCH, PATCH, WIDTH), (VARS * PATCH * PATCH) ** -0.5, 0.25),
        "embed_bias": gaussian(arg_keys[2], (WIDTH,), 0.5, 3.0, (), jnp.float32),
        "conv_weight": gaussian(arg_keys[3], (3, 3, WIDTH, WIDTH), (9 * WIDTH) ** -0.5, 0.0625),
        "conv_bias": gaussian(arg_keys[4], (WIDTH,), 0.5, 3.0, (), jnp.float32),
    }


def reference(raw_fields, embed_weight, embed_bias, conv_weight, conv_bias):
    count, height, breadth = raw_fields.shape
    patch_rows = height // PATCH
    patch_cols = breadth // PATCH
    grid_blocks = raw_fields.astype(jnp.float32).reshape(count, patch_rows, PATCH, patch_cols, PATCH)
    embedded = jnp.einsum("vaibj,vijd->abd", grid_blocks, embed_weight.astype(jnp.float32))
    embedded = (embedded + embed_bias).astype(jnp.bfloat16)
    channels = embedded.shape[2]
    padded = jnp.pad(embedded, ((0, 0), (1, 1), (0, 0)), mode="wrap")
    padded = jnp.pad(padded, ((1, 1), (0, 0), (0, 0)))
    summed = jnp.zeros((patch_rows * patch_cols, channels), jnp.float32)
    for step_row in range(3):
        for step_col in range(3):
            window = padded[step_row:step_row + patch_rows, step_col:step_col + patch_cols].reshape(-1, channels)
            summed = summed + jnp.dot(window, conv_weight[step_row, step_col], preferred_element_type=jnp.float32)
    summed = summed + conv_bias
    result = jax.nn.gelu(summed, approximate=False).astype(jnp.bfloat16)
    return result.reshape(patch_rows, patch_cols, channels)
```

```python
import functools

import jax
import jax.numpy as jnp
from jax import lax
from jax.experimental import pallas as pl
from jax.experimental.pallas import tpu as pltpu
from jax.sharding import PartitionSpec as P

PATCH = 4
LANES = 128
CELLS = PATCH * PATCH
MESH = pl.DeviceIdType.MESH


def kernel(
    dims,
    raw_hbm, ew_hbm, eb_ref, cw_hbm, cb_ref,
    out_ref,
    raw, field, sides, send, send_halo, recv, recv_halo, ew_raw, ew, cw, taps,
    raw_sem, ew_sem, cw_sem, send_sem, recv_sem, hsend_sem, hrecv_sem,
):
    lat_n, lon_n, height, breadth, rows, cols, width = dims
    total = lat_n * lon_n
    lat = lax.axis_index("lat")
    lon = lax.axis_index("lon")
    me = lat * lon_n + lon
    row_slots = taps.shape[0] // (rows + 2)
    spare = LANES - row_slots

    raw_copy = pltpu.make_async_copy(raw_hbm.at[0], raw, raw_sem)
    raw_copy.start()

    def peer(step):
        k = step // lon_n
        r = step % lon_n
        off = lat_n // 2 + (2 * (k % 2) - 1) * ((k + 1) // 2)
        return (lat + off + lat_n) % lat_n, (lon + r + 1) % lon_n

    barrier = pltpu.get_barrier_semaphore()

    @pl.loop(0, total - 1)
    def _(step):
        a, b = peer(step)
        pl.semaphore_signal(barrier, inc=1, device_id=(a, b), device_id_type=MESH)

    ew_copy = pltpu.make_async_copy(ew_hbm, ew_raw, ew_sem)
    ew_copy.start()
    cw_copies = []
    for p in range(3):
        for q in range(3):
            copy = pltpu.make_async_copy(cw_hbm.at[p, q], cw.at[p, q], cw_sem.at[3 * p + q])
            copy.start()
            cw_copies.append(copy)

    whole = pl.cdiv(breadth, LANES)
    patches = breadth // PATCH
    raw_copy.wait()
    main_lanes = (breadth // LANES) * LANES
    field[:, :main_lanes] = raw[:, :main_lanes]
    if main_lanes < breadth:
        tail = raw[:, main_lanes:]
        fill = jnp.zeros((height, whole * LANES - breadth), jnp.bfloat16)
        field[:, main_lanes:] = jnp.concatenate([tail, fill], axis=1)

    group = min(lat_n, 8)
    group_rows = group * rows * PATCH
    block = group * CELLS
    lane = lax.broadcasted_iota(jnp.int32, (1, PATCH * LANES), 1)
    slot = lane % LANES
    cell = lane // LANES
    m = lax.broadcasted_iota(jnp.int32, (rows * block, 1), 0)
    target = (
        (m % PATCH) * group_rows
        + ((m // CELLS) % group) * (rows * PATCH)
        + (m // block) * PATCH
        + (m // PATCH) % PATCH
    )
    c = lax.broadcasted_iota(jnp.int32, (rows * block, PATCH * group_rows), 1)
    pick_rows = jnp.where(c == target, 1.0, 0.0).astype(jnp.bfloat16)
    for g in range(lat_n // group):
        band = field[g * group_rows : (g + 1) * group_rows, :]
        for l in range(lon_n):
            wanted = [
                (PATCH * ((cols * l - 1 + s) % patches)) // LANES for s in range(cols + 2)
            ]
            used = sorted(set(wanted))
            used += [
                b for b in sorted({(PATCH * ((cols * l - 1 + s) % patches) + PATCH - 1) // LANES for s in range(cols + 2)})
                if b not in used
            ]
            patch = (cols * l - 1 + slot + patches) % patches
            column = jnp.where(slot < cols + 2, PATCH * patch + cell, -1)
            picks = []
            parts = []
            for b in used:
                k = lax.broadcasted_iota(jnp.int32, (LANES, PATCH * LANES), 0) + b * LANES
                picks.append(jnp.where(k == column, 1.0, 0.0).astype(jnp.bfloat16))
                parts.append(band[:, b * LANES : (b + 1) * LANES])
            found = jnp.dot(
                jnp.concatenate(parts, axis=1),
                jnp.concatenate(picks, axis=0),
                preferred_element_type=jnp.float32,
            ).astype(jnp.bfloat16)
            for j in range(PATCH):
                sides[j * group_rows : (j + 1) * group_rows, l * LANES : (l + 1) * LANES] = (
                    found[:, j * LANES : (j + 1) * LANES]
                )
        tiles = jnp.dot(pick_rows, sides[...], preferred_element_type=jnp.float32)
        low = lax.broadcasted_iota(jnp.int32, (block, LANES), 1) < row_slots
        for l in range(lon_n):
            column = tiles[:, l * LANES : (l + 1) * LANES]
            per_row = [column[a * block : (a + 1) * block] for a in range(rows)]
            last = per_row[rows - 1]
            for a in range(rows - 1):
                moved = last if a * spare >= row_slots else pltpu.roll(
                    last, row_slots - a * spare, 1
                )
                packed = jnp.where(low, per_row[a], moved).astype(jnp.bfloat16)
                send[g * group : (g + 1) * group, l, :, a * LANES : (a + 1) * LANES] = (
                    packed.reshape(group, CELLS, LANES)
                )
            first = per_row[0].astype(jnp.bfloat16).reshape(group, CELLS, LANES)
            final = last.astype(jnp.bfloat16).reshape(group, CELLS, LANES)
            send_halo[g * group + 1 : (g + 1) * group + 1, l, :, :LANES] = final
            if g == 0:
                send_halo[0, l, :, :LANES] = jnp.zeros((CELLS, LANES), jnp.bfloat16)
                send_halo[: group - 1, l, :, LANES:] = first[1:]
            else:
                send_halo[g * group - 1 : (g + 1) * group - 1, l, :, LANES:] = first
            if g == lat_n // group - 1:
                send_halo[lat_n - 1, l, :, LANES:] = jnp.zeros((CELLS, LANES), jnp.bfloat16)

    pl.semaphore_wait(barrier, total - 1)

    def exchange(source, dest, out_sem, in_sem):
        @pl.loop(0, total - 1)
        def _(step):
            a, b = peer(step)
            pltpu.make_async_remote_copy(
                src_ref=source.at[a, b],
                dst_ref=dest.at[me],
                send_sem=out_sem,
                recv_sem=in_sem,
                device_id=(a, b),
                device_id_type=MESH,
            ).start()

        pltpu.make_async_copy(source.at[lat, lon], dest.at[me], in_sem).start()

    exchange(send, recv, send_sem, recv_sem)

    ew_copy.wait()
    for i in range(PATCH):
        ew[:, PATCH * i : PATCH * (i + 1), :] = ew_raw[:, i]
    pltpu.make_async_copy(recv, recv, recv_sem).wait()
    exchange(send_halo, recv_halo, hsend_sem, hrecv_sem)

    def place(row, n, tokens):
        lanes = slice(n, n + tokens.shape[1])
        start = row * row_slots
        for q in range(3):
            shifted = tokens if q == 0 else pltpu.roll(tokens, row_slots - q, 0)
            taps[start : start + row_slots, q * width + lanes.start : q * width + lanes.stop] = (
                shifted.astype(jnp.bfloat16)
            )

    step_n = 256
    x = recv[...].reshape(total * CELLS, recv.shape[2]).T
    for n in range(0, width, step_n):
        weights = ew[:, :, n : n + step_n].reshape(total * CELLS, step_n)
        e = jnp.dot(x, weights, preferred_element_type=jnp.float32) + eb_ref[:, n : n + step_n]
        chunks = []
        for a in range(rows - 1):
            place(a + 1, n, e[a * LANES : a * LANES + row_slots])
            if a * spare < row_slots:
                chunks.append(e[a * LANES + row_slots : (a + 1) * LANES])
        place(rows, n, jnp.concatenate(chunks, axis=0)[:row_slots])

    for copy in cw_copies:
        copy.wait()

    def conv(first_rows):
        @pl.loop(0, width // step_n)
        def _(block_n):
            n = pl.multiple_of(block_n * step_n, step_n)
            summed = None
            for p in range(3):
                spans = [
                    taps[(a + p) * row_slots : (a + p + count) * row_slots, :]
                    for a, count in first_rows
                ]
                left = spans[0] if len(spans) == 1 else jnp.concatenate(spans, axis=0)
                weights = cw[p, :, :, pl.ds(n, step_n)].reshape(3 * width, step_n)
                part = jnp.dot(left, weights, preferred_element_type=jnp.float32)
                summed = part if summed is None else summed + part
            summed = summed + cb_ref[:, pl.ds(n, step_n)]
            result = 0.5 * summed * (1.0 + lax.erf(summed * (0.5 ** 0.5)))
            result = result.astype(jnp.bfloat16)
            at = 0
            for a, count in first_rows:
                for k in range(count):
                    out_ref[a + k, :, pl.ds(n, step_n)] = result[at : at + cols]
                    at += row_slots

    conv([(1, rows - 2)])

    pltpu.make_async_copy(recv_halo, recv_halo, hrecv_sem).wait()
    x = recv_halo[...].reshape(total * CELLS, recv_halo.shape[2]).T
    top = jnp.where(lat > 0, 1.0, 0.0)
    bottom = jnp.where(lat < lat_n - 1, 1.0, 0.0)
    for n in range(0, width, step_n):
        weights = ew[:, :, n : n + step_n].reshape(total * CELLS, step_n)
        e = jnp.dot(x, weights, preferred_element_type=jnp.float32) + eb_ref[:, n : n + step_n]
        place(0, n, e[:row_slots] * top)
        place(rows + 1, n, e[LANES : LANES + row_slots] * bottom)
    conv([(0, 1), (rows - 1, 1)])

    sent = pl.ds(0, total - 1)
    pltpu.make_async_copy(recv.at[sent], recv.at[sent], send_sem).wait()
    pltpu.make_async_copy(recv_halo.at[sent], recv_halo.at[sent], hsend_sem).wait()


def per_device(raw_fields, embed_weight, embed_bias, conv_weight, conv_bias):
    lat_n = lax.axis_size("lat")
    lon_n = lax.axis_size("lon")
    total = lat_n * lon_n
    var_dev, height, breadth = raw_fields.shape
    assert var_dev == 1
    rows = height // lat_n // PATCH
    cols = breadth // lon_n // PATCH
    width = embed_weight.shape[3]
    row_slots = (cols + 2 + 15) // 16 * 16
    spare = LANES - row_slots
    assert row_slots < LANES and spare * (rows - 1) >= cols + 2
    dims = (lat_n, lon_n, height, breadth, rows, cols, width)
    group = min(lat_n, 8)
    bf16 = jnp.bfloat16
    whole = pl.cdiv(breadth, LANES) * LANES
    any_space = pl.BlockSpec(memory_space=pl.ANY)
    vmem = pl.BlockSpec(memory_space=pltpu.VMEM)
    return pl.pallas_call(
        functools.partial(kernel, dims),
        out_shape=jax.ShapeDtypeStruct((rows, cols, width), bf16),
        in_specs=[any_space, any_space, vmem, any_space, vmem],
        out_specs=vmem,
        scratch_shapes=[
            pltpu.VMEM((height, breadth), bf16),
            pltpu.VMEM((height, whole), bf16),
            pltpu.VMEM((PATCH * group * rows * PATCH, lon_n * LANES), bf16),
            pltpu.VMEM((lat_n, lon_n, CELLS, (rows - 1) * LANES), bf16),
            pltpu.VMEM((lat_n + 1, lon_n, CELLS, 2 * LANES), bf16),
            pltpu.VMEM((total, CELLS, (rows - 1) * LANES), bf16),
            pltpu.VMEM((total, CELLS, 2 * LANES), bf16),
            pltpu.VMEM((total, PATCH, PATCH, width), bf16),
            pltpu.VMEM((total, CELLS, width), bf16),
            pltpu.VMEM((3, 3, width, width), bf16),
            pltpu.VMEM(((rows + 2) * row_slots, 3 * width), bf16),
            pltpu.SemaphoreType.DMA,
            pltpu.SemaphoreType.DMA,
            pltpu.SemaphoreType.DMA((9,)),
            pltpu.SemaphoreType.DMA,
            pltpu.SemaphoreType.DMA,
            pltpu.SemaphoreType.DMA,
            pltpu.SemaphoreType.DMA,
        ],
        compiler_params=pltpu.CompilerParams(
            collective_id=0, has_side_effects=True, vmem_limit_bytes=60 * 1024 * 1024
        ),
        name="tiles",
    )(
        raw_fields,
        embed_weight,
        embed_bias.reshape(1, width),
        conv_weight,
        conv_bias.reshape(1, width),
    )


def solution(mesh):
    return jax.shard_map(
        per_device,
        mesh=mesh,
        in_specs=(P(("lat", "lon"), None, None), P(), P(), P(), P()),
        out_specs=P("lat", "lon", None),
        check_vma=False,
    )
```

```python
import functools

import jax
import jax.numpy as jnp
from jax import lax
from jax.experimental import pallas as pl
from jax.experimental.pallas import tpu as pltpu
from jax.sharding import PartitionSpec as P

PATCH = 4
LANES = 128
CELLS = PATCH * PATCH
MESH = pl.DeviceIdType.MESH


def kernel(
    dims,
    raw_hbm, ew_hbm, eb_hbm, cw_hbm, cb_hbm,
    out_ref,
    eb_ref, cb_ref, raw, sides, send, send_far, recv, recv_far, near, ew_raw, ew, cw, comb, bias, taps,
    eb_sem, cb_sem, raw_sem, ew_sem, cw_sem, send_sem, recv_sem, fsend_sem, frecv_sem, nsend_sem, nrecv_sem,
):
    lat_n, lon_n, height, breadth, rows, cols, width = dims
    total = lat_n * lon_n
    lat = lax.axis_index("lat")
    lon = lax.axis_index("lon")
    me = lat * lon_n + lon
    row_slots = taps.shape[0] // (rows + 2)
    composed = total * CELLS <= width
    tap_width = total * CELLS if composed else width
    spare = LANES - row_slots

    raw_copy = pltpu.make_async_copy(raw_hbm.at[0], raw, raw_sem)
    raw_copy.start()

    def peer(step):
        k = step // lon_n
        r = step % lon_n
        off = lat_n // 2 + (2 * (k % 2) - 1) * ((k + 1) // 2)
        return (lat + off + lat_n) % lat_n, (lon + r + 1) % lon_n

    barrier = pltpu.get_barrier_semaphore()

    @pl.loop(0, total - 1)
    def _(step):
        a, b = peer(step)
        pl.semaphore_signal(barrier, inc=1, device_id=(a, b), device_id_type=MESH)

    ew_copy = pltpu.make_async_copy(ew_hbm, ew_raw, ew_sem)
    ew_copy.start()
    bias_copies = [
        pltpu.make_async_copy(eb_hbm, eb_ref, eb_sem),
        pltpu.make_async_copy(cb_hbm, cb_ref, cb_sem),
    ]
    for copy in bias_copies:
        copy.start()
    cw_copies = []
    for p in range(3):
        for q in range(3):
            copy = pltpu.make_async_copy(cw_hbm.at[p, q], cw.at[p, q], cw_sem.at[3 * p + q])
            copy.start()
            cw_copies.append(copy)

    patches = breadth // PATCH
    group = min(lat_n, 8)
    group_rows = group * rows * PATCH
    block = group * CELLS
    lane = lax.broadcasted_iota(jnp.int32, (1, PATCH * LANES), 1)
    slot = lane % LANES
    cell = lane // LANES
    m = lax.broadcasted_iota(jnp.int32, (rows * block, 1), 0)
    target = (
        (m % PATCH) * group_rows
        + ((m // CELLS) % group) * (rows * PATCH)
        + (m // block) * PATCH
        + (m // PATCH) % PATCH
    )
    c = lax.broadcasted_iota(jnp.int32, (rows * block, PATCH * group_rows), 1)
    pick_rows = jnp.where(c == target, 1.0, 0.0).astype(jnp.bfloat16)
    pickers = []
    for l in range(lon_n):
        wanted = [PATCH * ((cols * l - 1 + s) % patches) for s in range(cols + 2)]
        used = sorted({x // LANES for w in wanted for x in (w, w + PATCH - 1)})
        patch = (cols * l - 1 + slot + patches) % patches
        column = jnp.where(slot < cols + 2, PATCH * patch + cell, -1)
        picks = []
        for b in used:
            k = lax.broadcasted_iota(jnp.int32, (LANES, PATCH * LANES), 0) + b * LANES
            picks.append(jnp.where(k == column, 1.0, 0.0).astype(jnp.bfloat16))
        pickers.append((used, jnp.concatenate(picks, axis=0)))
    raw_copy.wait()
    for g in range(lat_n // group):
        for l in range(lon_n):
            used, picks = pickers[l]
            parts = []
            for b in used:
                part = raw[
                    g * group_rows : (g + 1) * group_rows,
                    b * LANES : min((b + 1) * LANES, breadth),
                ]
                short = LANES - part.shape[1]
                if short:
                    fill = jnp.zeros((group_rows, short), jnp.bfloat16)
                    part = jnp.concatenate([part, fill], axis=1)
                parts.append(part)
            found = jnp.dot(
                jnp.concatenate(parts, axis=1), picks, preferred_element_type=jnp.float32
            ).astype(jnp.bfloat16)
            for j in range(PATCH):
                sides[j * group_rows : (j + 1) * group_rows, l * LANES : (l + 1) * LANES] = (
                    found[:, j * LANES : (j + 1) * LANES]
                )
        tiles = jnp.dot(pick_rows, sides[...], preferred_element_type=jnp.float32)
        low = lax.broadcasted_iota(jnp.int32, (block, LANES), 1) < row_slots
        for l in range(lon_n):
            column = tiles[:, l * LANES : (l + 1) * LANES]
            per_row = [column[a * block : (a + 1) * block] for a in range(rows)]
            spread = per_row[rows - 2]
            for k in range(rows - 1):
                moved = spread if k * spare >= row_slots else pltpu.roll(
                    spread, row_slots - k * spare, 1
                )
                kept = per_row[k if k < rows - 2 else rows - 1]
                packed = jnp.where(low, kept, moved).astype(jnp.bfloat16)
                send[g * group : (g + 1) * group, l, :, k * LANES : (k + 1) * LANES] = (
                    packed.reshape(group, CELLS, LANES)
                )
            first = per_row[0].astype(jnp.bfloat16).reshape(group, CELLS, LANES)
            final = per_row[rows - 1].astype(jnp.bfloat16).reshape(group, CELLS, LANES)
            for t in range(group):
                to = g * group + (t + 1 if t % 2 else t - 1)
                if 0 <= to < lat_n:
                    send_far[to, l] = final[t] if t % 2 else first[t]
            for t in (0, lat_n - 1):
                if t // group == g:
                    send_far[t, l] = jnp.zeros((CELLS, LANES), jnp.bfloat16)

    early = 0
    ew_copy.wait()
    for copy in bias_copies:
        copy.wait()
    for i in range(PATCH):
        ew[:total, PATCH * i : PATCH * (i + 1), :] = ew_raw[:, i]
    if composed:
        high = eb_ref[...].astype(jnp.bfloat16)
        rest = eb_ref[...] - high.astype(jnp.float32)
        index = lax.broadcasted_iota(jnp.int32, (CELLS, width), 0)
        both = jnp.where(index == 0, high.astype(jnp.float32), jnp.where(index == 1, rest, 0.0))
        ew[total] = both.astype(jnp.bfloat16)

        def compose(start, stop):
            @pl.loop(start, stop)
            def _(tap):
                p, q = tap // 3, tap % 3
                pltpu.make_async_copy(cw_hbm.at[p, q], cw.at[p, q], cw_sem.at[tap]).wait()
                left = ew[...].reshape((total + 1) * CELLS, width)
                for n in range(0, width, 256):
                    product = jnp.dot(
                        left, cw[p, q, :, n : n + 256], preferred_element_type=jnp.float32
                    )
                    comb[p, q, :, n : n + 256] = product[:tap_width].astype(jnp.bfloat16)
                    bias[tap, :, n : n + 256] = product[tap_width : tap_width + 8]

        compose(0, early)

    pl.semaphore_wait(barrier, total - 1)

    def exchange(source, dest, out_sem, in_sem):
        @pl.loop(0, total - 1)
        def _(step):
            a, b = peer(step)
            pltpu.make_async_remote_copy(
                src_ref=source.at[a, b],
                dst_ref=dest.at[me],
                send_sem=out_sem,
                recv_sem=in_sem,
                device_id=(a, b),
                device_id_type=MESH,
            ).start()

        pltpu.make_async_copy(source.at[lat, lon], dest.at[me], in_sem).start()

    exchange(send, recv, send_sem, recv_sem)

    if composed:
        compose(early, 9)

    pltpu.make_async_copy(recv, recv, recv_sem).wait()
    odd = lat % 2
    edge_tile = pl.multiple_of((rows - 2) * LANES * (1 - odd), LANES)
    pair_copy = pltpu.make_async_remote_copy(
        src_ref=recv.at[:, :, pl.ds(edge_tile, LANES)],
        dst_ref=near,
        send_sem=nsend_sem,
        recv_sem=nrecv_sem,
        device_id=(lat + 1 - 2 * odd, lon),
        device_id_type=MESH,
    )
    pair_copy.start()
    exchange(send_far, recv_far, fsend_sem, frecv_sem)

    def place(row, n, tokens):
        lanes = slice(n, n + tokens.shape[1])
        start = row * row_slots
        if not isinstance(start, int):
            start = pl.multiple_of(start, 16)
        for q in range(3):
            shifted = tokens if q == 0 else pltpu.roll(tokens, row_slots - q, 0)
            taps[pl.ds(start, row_slots), q * tap_width + lanes.start : q * tap_width + lanes.stop] = (
                shifted.astype(jnp.bfloat16)
            )

    step_n = 256
    kernel_weights = comb if composed else cw

    def embed(x, n):
        weights = ew[:total, :, n : n + step_n].reshape(total * CELLS, step_n)
        return jnp.dot(x, weights, preferred_element_type=jnp.float32) + eb_ref[:, n : n + step_n]

    x = recv[...].reshape(total * CELLS, recv.shape[2]).T
    for n in range(0, tap_width, step_n):
        e = x[:, n : n + step_n].astype(jnp.float32) if composed else embed(x, n)
        chunks = []
        for k in range(rows - 1):
            row = k if k < rows - 2 else rows - 1
            place(row + 1, n, e[k * LANES : k * LANES + row_slots])
            if k * spare < row_slots:
                chunks.append(e[k * LANES + row_slots : (k + 1) * LANES])
        place(rows - 1, n, jnp.concatenate(chunks, axis=0)[:row_slots])

    top = jnp.where(lat > 0, 1.0, 0.0)
    bottom = jnp.where(lat < lat_n - 1, 1.0, 0.0)
    if not composed:
        for copy in cw_copies:
            copy.wait()

    def row_bias(a, n):
        total_bias = cb_ref[:, pl.ds(n, step_n)]
        if composed:
            for p in range(3):
                part = 0.0
                for q in range(3):
                    part += bias[3 * p + q, 0:1, pl.ds(n, step_n)] + bias[3 * p + q, 1:2, pl.ds(n, step_n)]
                if a + p == 0:
                    part *= top
                if a + p == rows + 1:
                    part *= bottom
                total_bias = total_bias + part
        return total_bias

    def conv(first_rows):
        @pl.loop(0, width // (2 * step_n))
        def _(block_n):
            for half in range(2):
                n = pl.multiple_of(block_n * (2 * step_n) + half * step_n, step_n)
                summed = None
                for p in range(3):
                    spans = [
                        taps[(a + p) * row_slots : (a + p + count) * row_slots, :]
                        for a, count in first_rows
                    ]
                    left = spans[0] if len(spans) == 1 else jnp.concatenate(spans, axis=0)
                    weights = kernel_weights[p, :, :, pl.ds(n, step_n)]
                    weights = weights.reshape(3 * tap_width, step_n)
                    part = jnp.dot(left, weights, preferred_element_type=jnp.float32)
                    summed = part if summed is None else summed + part
                at = 0
                for a, count in first_rows:
                    shift = row_bias(a, n)
                    for k in range(count):
                        value = summed[at : at + row_slots] + shift
                        value = 0.5 * value * (1.0 + lax.erf(value * (0.5 ** 0.5)))
                        out_ref[a + k, :, pl.ds(n, step_n)] = value[:cols].astype(jnp.bfloat16)
                        at += row_slots

    conv([(1, rows - 2)])

    pair_copy.wait_recv()
    pltpu.make_async_copy(recv_far, recv_far, frecv_sem).wait()
    inside = top * bottom
    for source, row, scale in (
        (near, (rows + 1) * (1 - odd), None),
        (recv_far, (rows + 1) * odd, inside),
    ):
        x = source[...].reshape(total * CELLS, LANES).T[:row_slots]
        for n in range(0, tap_width, step_n):
            if composed:
                e = x[:, n : n + step_n].astype(jnp.float32)
            else:
                e = embed(x, n)
                e = e if scale is None else e * scale
            place(row, n, e)
    conv([(0, 1), (rows - 1, 1)])

    sent = pl.ds(0, total - 1)
    pltpu.make_async_copy(recv.at[sent], recv.at[sent], send_sem).wait()
    pltpu.make_async_copy(recv_far.at[sent], recv_far.at[sent], fsend_sem).wait()
    pair_copy.wait_send()


def per_device(raw_fields, embed_weight, embed_bias, conv_weight, conv_bias):
    lat_n = lax.axis_size("lat")
    lon_n = lax.axis_size("lon")
    total = lat_n * lon_n
    var_dev, height, breadth = raw_fields.shape
    assert var_dev == 1 and lat_n % 2 == 0
    rows = height // lat_n // PATCH
    cols = breadth // lon_n // PATCH
    width = embed_weight.shape[3]
    row_slots = (cols + 2 + 15) // 16 * 16
    spare = LANES - row_slots
    assert row_slots < LANES and spare * (rows - 1) >= cols + 2
    dims = (lat_n, lon_n, height, breadth, rows, cols, width)
    group = min(lat_n, 8)
    bf16 = jnp.bfloat16
    composed = total * CELLS <= width
    tap_width = total * CELLS if composed else width
    any_space = pl.BlockSpec(memory_space=pltpu.HBM)
    vmem = pl.BlockSpec(memory_space=pltpu.VMEM)
    return pl.pallas_call(
        functools.partial(kernel, dims),
        out_shape=jax.ShapeDtypeStruct((rows, cols, width), bf16),
        in_specs=[any_space]*5,
        out_specs=vmem,
        scratch_shapes=[
            pltpu.VMEM((1, width), jnp.float32),
            pltpu.VMEM((1, width), jnp.float32),
            pltpu.VMEM((height, breadth), bf16),
            pltpu.VMEM((PATCH * group * rows * PATCH, lon_n * LANES), bf16),
            pltpu.VMEM((lat_n, lon_n, CELLS, (rows - 1) * LANES), bf16),
            pltpu.VMEM((lat_n, lon_n, CELLS, LANES), bf16),
            pltpu.VMEM((total, CELLS, (rows - 1) * LANES), bf16),
            pltpu.VMEM((total, CELLS, LANES), bf16),
            pltpu.VMEM((total, CELLS, LANES), bf16),
            pltpu.VMEM((total, PATCH, PATCH, width), bf16),
            pltpu.VMEM((total + 1, CELLS, width), bf16),
            pltpu.VMEM((3, 3, width, width), bf16),
            pltpu.VMEM((3, 3, tap_width if composed else CELLS, width), bf16),
            pltpu.VMEM((9, 8, width), jnp.float32),
            pltpu.VMEM(((rows + 2) * row_slots, 3 * tap_width), bf16),
            pltpu.SemaphoreType.DMA,
            pltpu.SemaphoreType.DMA,
            pltpu.SemaphoreType.DMA,
            pltpu.SemaphoreType.DMA,
            pltpu.SemaphoreType.DMA((9,)),
            pltpu.SemaphoreType.DMA,
            pltpu.SemaphoreType.DMA,
            pltpu.SemaphoreType.DMA,
            pltpu.SemaphoreType.DMA,
            pltpu.SemaphoreType.DMA,
            pltpu.SemaphoreType.DMA,
        ],
        compiler_params=pltpu.CompilerParams(
            collective_id=0, has_side_effects=True, vmem_limit_bytes=52 * 1024 * 1024
        ),
        name="tiles",
    )(
        *(pltpu.with_memory_space_constraint(v, pltpu.HBM) for v in (raw_fields, embed_weight, embed_bias.reshape(1, width), conv_weight, conv_bias.reshape(1, width))),
    )


def solution(mesh):
    return jax.shard_map(
        per_device,
        mesh=mesh,
        in_specs=(P(("lat", "lon"), None, None), P(), P(), P(), P()),
        out_specs=P("lat", "lon", None),
        check_vma=False,
    )
```

```python
import functools

import jax
import jax.numpy as jnp
from jax import lax
from jax.experimental import pallas as pl
from jax.experimental.pallas import tpu as pltpu
from jax.sharding import PartitionSpec as P

PATCH = 4
LANES = 128
CELLS = PATCH * PATCH
MESH = pl.DeviceIdType.MESH


def kernel(
    dims,
    raw_hbm, ew_hbm, eb_hbm, cw_hbm, cb_hbm,
    out_ref,
    eb_ref, cb_ref, raw, sides, send, send_far, recv, recv_far, near, ew_raw, ew, cw, comb, bias, taps,
    eb_sem, cb_sem, raw_sem, ew_sem, cw_sem, send_sem, recv_sem, fsend_sem, frecv_sem, nsend_sem, nrecv_sem,
):
    lat_n, lon_n, height, breadth, rows, cols, width = dims
    total = lat_n * lon_n
    lat = lax.axis_index("lat")
    lon = lax.axis_index("lon")
    me = lat * lon_n + lon
    row_slots = taps.shape[0] // (rows + 2)
    composed = total * CELLS <= width
    tap_width = total * CELLS if composed else width
    spare = LANES - row_slots

    raw_copy = pltpu.make_async_copy(raw_hbm.at[0], raw, raw_sem)
    raw_copy.start()

    def peer(step):
        k = step // lon_n
        r = step % lon_n
        off = lat_n // 2 + (2 * (k % 2) - 1) * ((k + 1) // 2)
        return (lat + off + lat_n) % lat_n, (lon + r + 1) % lon_n

    barrier = pltpu.get_barrier_semaphore()

    @pl.loop(0, total - 1, unroll=total <= 32)
    def _(step):
        a, b = peer(step)
        pl.semaphore_signal(barrier, inc=1, device_id=(a, b), device_id_type=MESH)

    ew_copy = pltpu.make_async_copy(ew_hbm, ew_raw, ew_sem)
    ew_copy.start()
    bias_copies = [
        pltpu.make_async_copy(eb_hbm, eb_ref, eb_sem),
        pltpu.make_async_copy(cb_hbm, cb_ref, cb_sem),
    ]
    for copy in bias_copies:
        copy.start()
    cw_copies = []
    for p in range(3):
        for q in range(3):
            copy = pltpu.make_async_copy(cw_hbm.at[p, q], cw.at[p, q], cw_sem.at[3 * p + q])
            copy.start()
            cw_copies.append(copy)

    patches = breadth // PATCH
    group = min(lat_n, 8)
    group_rows = group * rows * PATCH
    block = group * CELLS
    lane = lax.broadcasted_iota(jnp.int32, (1, PATCH * LANES), 1)
    slot = lane % LANES
    cell = lane // LANES
    m = lax.broadcasted_iota(jnp.int32, (rows * block, 1), 0)
    target = (
        (m % PATCH) * group_rows
        + ((m // CELLS) % group) * (rows * PATCH)
        + (m // block) * PATCH
        + (m // PATCH) % PATCH
    )
    c = lax.broadcasted_iota(jnp.int32, (rows * block, PATCH * group_rows), 1)
    pick_rows = jnp.where(c == target, 1.0, 0.0).astype(jnp.bfloat16)
    pickers = []
    for l in range(lon_n):
        wanted = [PATCH * ((cols * l - 1 + s) % patches) for s in range(cols + 2)]
        used = sorted({x // LANES for w in wanted for x in (w, w + PATCH - 1)})
        patch = (cols * l - 1 + slot + patches) % patches
        column = jnp.where(slot < cols + 2, PATCH * patch + cell, -1)
        picks = []
        for b in used:
            k = lax.broadcasted_iota(jnp.int32, (LANES, PATCH * LANES), 0) + b * LANES
            picks.append(jnp.where(k == column, 1.0, 0.0).astype(jnp.bfloat16))
        pickers.append((used, jnp.concatenate(picks, axis=0)))
    raw_copy.wait()
    for g in range(lat_n // group):
        for l in range(lon_n):
            used, picks = pickers[l]
            parts = []
            for b in used:
                part = raw[
                    g * group_rows : (g + 1) * group_rows,
                    b * LANES : min((b + 1) * LANES, breadth),
                ]
                short = LANES - part.shape[1]
                if short:
                    fill = jnp.zeros((group_rows, short), jnp.bfloat16)
                    part = jnp.concatenate([part, fill], axis=1)
                parts.append(part)
            found = jnp.dot(
                jnp.concatenate(parts, axis=1), picks, preferred_element_type=jnp.float32
            ).astype(jnp.bfloat16)
            for j in range(PATCH):
                sides[j * group_rows : (j + 1) * group_rows, l * LANES : (l + 1) * LANES] = (
                    found[:, j * LANES : (j + 1) * LANES]
                )
        tiles = jnp.dot(pick_rows, sides[...], preferred_element_type=jnp.float32)
        low = lax.broadcasted_iota(jnp.int32, (block, LANES), 1) < row_slots
        for l in range(lon_n):
            column = tiles[:, l * LANES : (l + 1) * LANES]
            per_row = [column[a * block : (a + 1) * block] for a in range(rows)]
            spread = per_row[rows - 2]
            for k in range(rows - 1):
                moved = spread if k * spare >= row_slots else pltpu.roll(
                    spread, row_slots - k * spare, 1
                )
                kept = per_row[k if k < rows - 2 else rows - 1]
                packed = jnp.where(low, kept, moved).astype(jnp.bfloat16)
                send[g * group : (g + 1) * group, l, :, k * LANES : (k + 1) * LANES] = (
                    packed.reshape(group, CELLS, LANES)
                )
            first = per_row[0].astype(jnp.bfloat16).reshape(group, CELLS, LANES)
            final = per_row[rows - 1].astype(jnp.bfloat16).reshape(group, CELLS, LANES)
            for t in range(group):
                to = g * group + (t + 1 if t % 2 else t - 1)
                if 0 <= to < lat_n:
                    send_far[to, l] = final[t] if t % 2 else first[t]
            for t in (0, lat_n - 1):
                if t // group == g:
                    send_far[t, l] = jnp.zeros((CELLS, LANES), jnp.bfloat16)

    early = 0
    ew_copy.wait()
    for copy in bias_copies:
        copy.wait()
    for i in range(PATCH):
        ew[:total, PATCH * i : PATCH * (i + 1), :] = ew_raw[:, i]
    if composed:
        high = eb_ref[...].astype(jnp.bfloat16)
        rest = eb_ref[...] - high.astype(jnp.float32)
        index = lax.broadcasted_iota(jnp.int32, (CELLS, width), 0)
        both = jnp.where(index == 0, high.astype(jnp.float32), jnp.where(index == 1, rest, 0.0))
        ew[total] = both.astype(jnp.bfloat16)

        def compose(start, stop):
            @pl.loop(start, stop)
            def _(tap):
                p, q = tap // 3, tap % 3
                pltpu.make_async_copy(cw_hbm.at[p, q], cw.at[p, q], cw_sem.at[tap]).wait()
                left = ew[...].reshape((total + 1) * CELLS, width)
                for n in range(0, width, 256):
                    product = jnp.dot(
                        left, cw[p, q, :, n : n + 256], preferred_element_type=jnp.float32
                    )
                    comb[p, q, :, n : n + 256] = product[:tap_width].astype(jnp.bfloat16)
                    bias[tap, :, n : n + 256] = product[tap_width : tap_width + 8]

        compose(0, early)

    pl.semaphore_wait(barrier, total - 1)

    def exchange(source, dest, out_sem, in_sem):
        @pl.loop(0, total - 1, unroll=total <= 32)
        def _(step):
            a, b = peer(step)
            pltpu.make_async_remote_copy(
                src_ref=source.at[a, b],
                dst_ref=dest.at[me],
                send_sem=out_sem,
                recv_sem=in_sem,
                device_id=(a, b),
                device_id_type=MESH,
            ).start()

        pltpu.make_async_copy(source.at[lat, lon], dest.at[me], in_sem).start()

    exchange(send, recv, send_sem, recv_sem)

    if composed:
        compose(early, 9)

    pltpu.make_async_copy(recv, recv, recv_sem).wait()
    odd = lat % 2
    edge_tile = pl.multiple_of((rows - 2) * LANES * (1 - odd), LANES)
    pair_copy = pltpu.make_async_remote_copy(
        src_ref=recv.at[:, :, pl.ds(edge_tile, LANES)],
        dst_ref=near,
        send_sem=nsend_sem,
        recv_sem=nrecv_sem,
        device_id=(lat + 1 - 2 * odd, lon),
        device_id_type=MESH,
    )
    pair_copy.start()
    exchange(send_far, recv_far, fsend_sem, frecv_sem)

    def place(row, n, tokens):
        lanes = slice(n, n + tokens.shape[1])
        start = row * row_slots
        if not isinstance(start, int):
            start = pl.multiple_of(start, 16)
        for q in range(3):
            shifted = tokens if q == 0 else pltpu.roll(tokens, row_slots - q, 0)
            taps[pl.ds(start, row_slots), q * tap_width + lanes.start : q * tap_width + lanes.stop] = (
                shifted.astype(jnp.bfloat16)
            )

    step_n = 256
    kernel_weights = comb if composed else cw

    def embed(x, n):
        weights = ew[:total, :, n : n + step_n].reshape(total * CELLS, step_n)
        return jnp.dot(x, weights, preferred_element_type=jnp.float32) + eb_ref[:, n : n + step_n]

    x = recv[...].reshape(total * CELLS, recv.shape[2]).T
    for n in range(0, tap_width, step_n):
        e = x[:, n : n + step_n].astype(jnp.float32) if composed else embed(x, n)
        chunks = []
        for k in range(rows - 1):
            row = k if k < rows - 2 else rows - 1
            place(row + 1, n, e[k * LANES : k * LANES + row_slots])
            if k * spare < row_slots:
                chunks.append(e[k * LANES + row_slots : (k + 1) * LANES])
        place(rows - 1, n, jnp.concatenate(chunks, axis=0)[:row_slots])

    top = jnp.where(lat > 0, 1.0, 0.0)
    bottom = jnp.where(lat < lat_n - 1, 1.0, 0.0)
    if not composed:
        for copy in cw_copies:
            copy.wait()

    def row_bias(a, n, scales):
        total_bias = cb_ref[:, pl.ds(n, step_n)]
        if composed:
            for p in range(3):
                part = 0.0
                for q in range(3):
                    part += bias[3 * p + q, 0:1, pl.ds(n, step_n)] + bias[3 * p + q, 1:2, pl.ds(n, step_n)]
                if scales is not None:
                    part *= scales[p]
                total_bias = total_bias + part
        return total_bias

    def tap_rows(row, count):
        if isinstance(row, int):
            return taps[row * row_slots : (row + count) * row_slots, :]
        return taps[pl.ds(pl.multiple_of(row * row_slots, 16), count * row_slots), :]

    def conv(a, count, scales):
        @pl.loop(0, width // (2 * step_n))
        def _(block_n):
            for half in range(2):
                n = pl.multiple_of(block_n * (2 * step_n) + half * step_n, step_n)
                summed = None
                for p in range(3):
                    left = tap_rows(a + p, count)
                    weights = kernel_weights[p, :, :, pl.ds(n, step_n)]
                    weights = weights.reshape(3 * tap_width, step_n)
                    part = jnp.dot(left, weights, preferred_element_type=jnp.float32)
                    summed = part if summed is None else summed + part
                shift = row_bias(a, n, scales)
                for k in range(count):
                    value = summed[k * row_slots : (k + 1) * row_slots] + shift
                    value = 0.5 * value * (1.0 + lax.erf(value * (0.5 ** 0.5)))
                    out_ref[a + k, :, pl.ds(n, step_n)] = value[:cols].astype(jnp.bfloat16)

    conv(1, rows - 2, None)

    inside = top * bottom
    even = jnp.where(odd > 0, 0.0, 1.0)
    scales = (1.0 - even * (1.0 - inside), 1.0, 1.0 - (1.0 - even) * (1.0 - inside))

    def edge(source, below, factor, row_scales):
        x = source[...].reshape(total * CELLS, LANES).T[:row_slots]
        for n in range(0, tap_width, step_n):
            if composed:
                e = x[:, n : n + step_n].astype(jnp.float32)
            else:
                e = embed(x, n)
                e = e if factor is None else e * factor
            place((rows + 1) * below, n, e)
        conv((rows - 1) * below, 1, row_scales)

    pair_copy.wait_recv()
    edge(near, 1 - odd, None, None)
    pltpu.make_async_copy(recv_far, recv_far, frecv_sem).wait()
    edge(recv_far, odd, inside, scales)

    sent = pl.ds(0, total - 1)
    pltpu.make_async_copy(recv.at[sent], recv.at[sent], send_sem).wait()
    pltpu.make_async_copy(recv_far.at[sent], recv_far.at[sent], fsend_sem).wait()
    pair_copy.wait_send()


def per_device(raw_fields, embed_weight, embed_bias, conv_weight, conv_bias):
    lat_n = lax.axis_size("lat")
    lon_n = lax.axis_size("lon")
    total = lat_n * lon_n
    var_dev, height, breadth = raw_fields.shape
    assert var_dev == 1 and lat_n % 2 == 0
    rows = height // lat_n // PATCH
    cols = breadth // lon_n // PATCH
    width = embed_weight.shape[3]
    row_slots = (cols + 2 + 15) // 16 * 16
    spare = LANES - row_slots
    assert row_slots < LANES and spare * (rows - 1) >= cols + 2
    dims = (lat_n, lon_n, height, breadth, rows, cols, width)
    group = min(lat_n, 8)
    bf16 = jnp.bfloat16
    composed = total * CELLS <= width
    tap_width = total * CELLS if composed else width
    any_space = pl.BlockSpec(memory_space=pltpu.HBM)
    vmem = pl.BlockSpec(memory_space=pltpu.VMEM)
    return pl.pallas_call(
        functools.partial(kernel, dims),
        out_shape=jax.ShapeDtypeStruct((rows, cols, width), bf16),
        in_specs=[any_space]*5,
        out_specs=vmem,
        scratch_shapes=[
            pltpu.VMEM((1, width), jnp.float32),
            pltpu.VMEM((1, width), jnp.float32),
            pltpu.VMEM((height, breadth), bf16),
            pltpu.VMEM((PATCH * group * rows * PATCH, lon_n * LANES), bf16),
            pltpu.VMEM((lat_n, lon_n, CELLS, (rows - 1) * LANES), bf16),
            pltpu.VMEM((lat_n, lon_n, CELLS, LANES), bf16),
            pltpu.VMEM((total, CELLS, (rows - 1) * LANES), bf16),
            pltpu.VMEM((total, CELLS, LANES), bf16),
            pltpu.VMEM((total, CELLS, LANES), bf16),
            pltpu.VMEM((total, PATCH, PATCH, width), bf16),
            pltpu.VMEM((total + 1, CELLS, width), bf16),
            pltpu.VMEM((3, 3, width, width), bf16),
            pltpu.VMEM((3, 3, tap_width if composed else CELLS, width), bf16),
            pltpu.VMEM((9, 8, width), jnp.float32),
            pltpu.VMEM(((rows + 2) * row_slots, 3 * tap_width), bf16),
            pltpu.SemaphoreType.DMA,
            pltpu.SemaphoreType.DMA,
            pltpu.SemaphoreType.DMA,
            pltpu.SemaphoreType.DMA,
            pltpu.SemaphoreType.DMA((9,)),
            pltpu.SemaphoreType.DMA,
            pltpu.SemaphoreType.DMA,
            pltpu.SemaphoreType.DMA,
            pltpu.SemaphoreType.DMA,
            pltpu.SemaphoreType.DMA,
            pltpu.SemaphoreType.DMA,
        ],
        compiler_params=pltpu.CompilerParams(
            collective_id=0, has_side_effects=True, vmem_limit_bytes=52 * 1024 * 1024
        ),
        name="tiles",
    )(
        *(pltpu.with_memory_space_constraint(v, pltpu.HBM) for v in (raw_fields, embed_weight, embed_bias.reshape(1, width), conv_weight, conv_bias.reshape(1, width))),
    )


def solution(mesh):
    return jax.shard_map(
        per_device,
        mesh=mesh,
        in_specs=(P(("lat", "lon"), None, None), P(), P(), P(), P()),
        out_specs=P("lat", "lon", None),
        check_vma=False,
    )
```
